512 devices in a mesh: dp: 128 (over x, y, z_hi, core), tensor: 4 (over z_lo).
Axes of the slice: x: 4, y: 8, z: 8 (z_hi: 2, z_lo: 4; z = z_hi * 4 + z_lo), core: 2. Of those that a mesh axis runs over, the one named last changes fastest.
Arguments:
- inputs_x: bfloat16 [16384, 4096], P('dp', 'tensor'), may hold values from -6 to 6
- hidden: bfloat16 [16384, 14336], P('dp', 'tensor'), may hold values from -6 to 6
- grad_up: bfloat16 [16384, 14336], P('dp', 'tensor'), may hold values from -6 to 6
- grad_down: bfloat16 [16384, 4096], P('dp', 'tensor'), may hold values from -6 to 6
- proj_in_up: bfloat16 [4096, 64], P('tensor'), may hold values from -0.09375 to 0.09375
- proj_in_down: bfloat16 [14336, 64], P('tensor'), may hold values from -0.046875 to 0.046875
- proj_out_up: bfloat16 [14336, 64], P('tensor'), may hold values from -0.046875 to 0.046875
- proj_out_down: bfloat16 [4096, 64], P('tensor'), may hold values from -0.09375 to 0.09375
- lengths: int32 [256], P('dp'), may hold values from 16 to 64
- stored_grads: bfloat16 [3328, 8192], P('dp', 'tensor'), may hold values from -6 to 6
Outputs:
- gram: bfloat16 [8192, 128, 64], P('tensor', 'dp')
The draws below stay inside these ranges and needn't reach their ends.
All inputs are finite; a program needn't handle non-finite values.
Results may differ from the reference program's by a relative error of at most 0.0034.
Values may be sent and summed in bfloat16 or wider, within the bound.
A program may use at most 64 MiB of HBM per device.

```python
import math
import jax
import jax.numpy as jnp
from jax import lax

D = 4096
FF = 14336
K = 64
LAYERS = 2
SLOTS = 64
EXAMPLES = 256
TOKENS = 16384
STORED = 3328
FEAT = 8192
N_DP = 128
N_TENSOR = 4


def place_ends(entries, own_key, smallest, largest):
    place = [jax.random.randint(jax.random.fold_in(own_key, axis), (), 0, length) for axis, length in enumerate(entries.shape)]
    widest = entries.shape.index(max(entries.shape))
    beside = place[:widest] + [(place[widest] + 1) % entries.shape[widest]] + place[widest + 1:]
    return entries.at[tuple(place)].set(smallest).at[tuple(beside)].set(largest)


def block_scale(rng, extent, cuts, low, top_value):
    def one(axis_at, shards_of):
        steps = jax.random.uniform(jax.random.fold_in(jax.random.fold_in(rng, 6), axis_at), (shards_of,), jnp.float32, low / len(cuts), top_value / len(cuts))
        return jnp.repeat(jnp.exp(steps), extent[axis_at] // shards_of).reshape((-1,) + (1,) * (len(extent) - axis_at - 1))

    loudness = one(*cuts[0])
    for cut in cuts[1:]:
        loudness = loudness * one(*cut)
    return loudness


def noise(own_key, extent, deviation, reach, pieces=(), kind=jnp.bfloat16):
    drawn = deviation * jax.random.normal(own_key, extent, jnp.float32)
    if pieces:
        drawn = drawn * block_scale(own_key, extent, pieces, -0.22, 0.18)
    return jnp.clip(drawn, -reach, reach).astype(kind)


def setup_inputs(seed: int = 0) -> dict:
    key_list = jax.random.split(jax.random.key(seed), 11)
    inputs_x = noise(key_list[0], (TOKENS, D), 1.0, 6.0, ((0, 128), (1, 4)))
    hidden = noise(key_list[1], (TOKENS, FF), 1.0, 6.0, ((0, 128), (1, 4)))
    grad_up = noise(key_list[2], (TOKENS, FF), 1.0, 6.0, ((0, 128), (1, 4)))
    grad_down = noise(key_list[3], (TOKENS, D), 1.0, 6.0, ((0, 128), (1, 4)))
    proj_in_up = noise(key_list[4], (D, K), D ** -0.5, 0.09375, ((0, 4),))
    proj_in_down = noise(key_list[5], (FF, K), FF ** -0.5, 0.046875, ((0, 4),))
    proj_out_up = noise(key_list[6], (FF, K), FF ** -0.5, 0.046875, ((0, 4),))
    proj_out_down = noise(key_list[7], (D, K), D ** -0.5, 0.09375, ((0, 4),))
    lengths = place_ends(jax.random.randint(key_list[8], (EXAMPLES,), SLOTS // 4, SLOTS + 1), jax.random.fold_in(key_list[8], 1), SLOTS // 4, SLOTS).astype(jnp.int32)
    stored_grads = noise(key_list[9], (STORED, FEAT), 1.0, 6.0, ((0, 128), (1, 4)))
    return {"inputs_x": inputs_x, "hidden": hidden, "grad_up": grad_up, "grad_down": grad_down, "proj_in_up": proj_in_up, "proj_in_down": proj_in_down, "proj_out_up": proj_out_up, "proj_out_down": proj_out_down, "lengths": lengths, "stored_grads": stored_grads}


def matmul(left, right):
    return jnp.dot(left, right, preferred_element_type=jnp.float32)

def reference(inputs_x, hidden, grad_up, grad_down, proj_in_up, proj_in_down, proj_out_up, proj_out_down, lengths, stored_grads):
    examples = lengths.shape[0]
    live_mask = (jnp.arange(SLOTS, dtype=jnp.int32)[None, :] < lengths[:, None]).astype(jnp.float32)
    in_proj = jnp.stack([matmul(inputs_x, proj_in_up), matmul(hidden, proj_in_down)], axis=1)
    out_proj = jnp.stack([matmul(grad_up, proj_out_up), matmul(grad_down, proj_out_down)], axis=1)
    in_proj = in_proj.reshape(examples, SLOTS, LAYERS, K)
    out_proj = out_proj.reshape(examples, SLOTS, LAYERS, K) * live_mask[:, :, None, None]
    current = jnp.einsum('esla,eslb->ealb', out_proj, in_proj, precision=lax.Precision.HIGHEST)
    current = (current * (1.0 / math.sqrt(SLOTS))).reshape(examples, FEAT).astype(jnp.bfloat16)
    rows = jnp.concatenate([current, stored_grads], axis=0)
    full = lax.dot_general(rows, rows, (((0,), (0,)), ((), ())), preferred_element_type=jnp.float32)
    full = full * (1.0 / math.sqrt(rows.shape[0]))
    quarter = FEAT // N_TENSOR
    sub_width = quarter // N_DP
    gram = full.reshape(FEAT, N_TENSOR, N_DP, sub_width).transpose(0, 2, 1, 3)
    return gram.reshape(FEAT, N_DP, N_TENSOR * sub_width).astype(jnp.bfloat16)
```

```python
import functools
import math

import jax
import jax.numpy as jnp
from jax import lax
from jax.experimental import pallas as pl
from jax.experimental.pallas import tpu as pltpu
from jax.sharding import PartitionSpec as P

MESH = pl.DeviceIdType.MESH
NX, NY, NH, NC, NT = 4, 8, 2, 2, 4


def matmul(left, right):
    return jnp.dot(left, right, preferred_element_type=jnp.float32)


def exchange(scale, lrow, rcol, out, la, rb, acc, cr, obuf,
             a1s, a1r, b1s, b1r, ts, tr, xs, xr, ys, yr, cs_s, cs_r, os_, or_, loc):
    d = lax.axis_index("dp")
    t = lax.axis_index("tensor")
    x, y, h, c = d // 32, (d // 4) % 8, (d // 2) % 2, d % 2
    slot = rcol.shape[1]

    def dev(dx=0, dy=0, dh=0, dc=0, dt=0):
        xx, yy, hh, cc = (x + dx) % NX, (y + dy) % NY, (h + dh) % NH, (c + dc) % NC
        return (((xx * NY + yy) * NH + hh) * NC + cc, (t + dt) % NT)

    def remote(src, dst, ss, rs, to):
        return pltpu.make_async_remote_copy(
            src_ref=src, dst_ref=dst, send_sem=ss, recv_sem=rs, device_id=to, device_id_type=MESH
        )

    barrier = pltpu.get_barrier_semaphore()
    partners = [dev(dx=i, dh=k) for i in range(1, NX) for k in range(NH)]
    partners += [dev(dy=i, dh=k) for i in range(NY) for k in range(NH) if i or k]
    partners += [dev(dt=k) for k in range(1, NT)] + [dev(dc=1)]
    for p in partners:
        pl.semaphore_signal(barrier, inc=1, device_id=p, device_id_type=MESH)
    pl.semaphore_wait(barrier, len(partners))

    sends = []

    def go(copy):
        copy.start()
        sends.append(copy)

    def lanes(k):
        return pl.ds(pl.multiple_of(((t - k) % NT) * 128, 128), 128)

    own_l = pltpu.make_async_copy(lrow.at[x], la.at[y, h, x], loc.at[0])
    own_l.start()
    own_r = pltpu.make_async_copy(rcol.at[y * 2 + h], rb.at[x, y * 2 + h, :, lanes(0)], loc.at[1])
    own_r.start()
    for k in range(NH):
        for i in range(NX):
            if i or k:
                go(remote(lrow.at[(x + i) % NX], la.at[y, h, x], a1s.at[i * 2 + k],
                          a1r.at[i * 2 + k], dev(dx=i, dh=k)))
        for i in range(NY):
            if i or k:
                go(remote(rcol.at[((y + i) % NY) * 2 + (h + k) % 2],
                          rb.at[x, y * 2 + h, :, lanes(0)], b1s.at[i * 2 + k],
                          b1r.at[i * 2 + k], dev(dy=i, dh=k)))

    def a1_wait(i, k):
        dst = la.at[y, (h + k) % 2, (x - i) % NX]
        remote(dst, dst, a1s.at[i * 2 + k], a1r.at[i * 2 + k], dev(dx=i, dh=k)).wait_recv()

    def b1_wait(i, k):
        dst = rb.at[x, ((y - i) % NY) * 2 + (h + k) % 2, :, lanes(0)]
        remote(dst, dst, b1s.at[i * 2 + k], b1r.at[i * 2 + k], dev(dy=i, dh=k)).wait_recv()

    def y_last(way, j):
        return 3 if way == j else 2

    def y_send(way, j, s):
        sign = 1 - 2 * way
        ref = la.at[(y - sign * s) % NY, (h + j) % 2]
        i = (way * 2 + j) * 4 + s
        go(remote(ref, ref, ys.at[i], yr.at[i], dev(dy=sign)))

    def y_wait(way, j, s):
        sign = 1 - 2 * way
        ref = la.at[(y - sign * (s + 1)) % NY, (h + j) % 2]
        i = (way * 2 + j) * 4 + s
        remote(ref, ref, ys.at[i], yr.at[i], dev(dy=sign)).wait_recv()

    def y_step(j, s):
        for way in range(2):
            if s <= y_last(way, j):
                y_wait(way, j, s)
                if s + 1 <= y_last(way, j):
                    y_send(way, j, s + 1)

    def x_piece(way, k, s, at):
        sign = 1 - 2 * way
        col = (x - sign * at) % NX
        if s == 0:
            return rb.at[col, :, :, lanes(k)]
        return rb.at[col, pl.ds(8 * way, 8), :, lanes(k)]

    def x_send(way, k, s):
        ref = x_piece(way, k, s, s)
        i = (way * 4 + k) * 2 + s
        go(remote(ref, ref, xs.at[i], xr.at[i], dev(dx=1 - 2 * way)))

    def x_wait(way, k, s):
        ref = x_piece(way, k, s, s + 1)
        i = (way * 4 + k) * 2 + s
        remote(ref, ref, xs.at[i], xr.at[i], dev(dx=1 - 2 * way)).wait_recv()

    def t_wait(k):
        ref = rb.at[x, :, :, lanes(k)]
        remote(ref, ref, ts.at[k], tr.at[k], dev(dt=k)).wait_recv()
        for way in range(2):
            x_send(way, k, 0)

    def x_forward(k):
        for way in range(2):
            x_wait(way, k, 0)
            x_send(way, k, 1)

    own_l.wait()
    for i in range(1, NX):
        a1_wait(i, 0)
    for way in range(2):
        y_send(way, 0, 0)
    own_r.wait()
    for k in range(NH):
        for i in range(NY):
            if i or k:
                b1_wait(i, k)
    for k in range(1, NT):
        ref = rb.at[x, :, :, lanes(0)]
        go(remote(ref, ref, ts.at[k], tr.at[k], dev(dt=k)))
    for way in range(2):
        x_send(way, 0, 0)
    for i in range(NX):
        a1_wait(i, 1)
    for way in range(2):
        y_send(way, 1, 0)
    y_step(0, 0)
    x_forward(0)
    t_wait(1)
    y_step(1, 0)
    t_wait(3)
    t_wait(2)
    y_step(0, 1)
    x_forward(1)
    y_step(1, 1)
    x_forward(3)
    y_step(0, 2)
    x_forward(2)
    y_step(1, 2)
    for k in (0, 1, 3, 2):
        for way in range(2):
            x_wait(way, k, 1)
    y_step(0, 3)
    y_step(1, 3)

    def one(i, _):
        left = rb[i].reshape(16 * slot, 512)
        right = la[:, :, i].reshape(16 * slot, 512)
        part = lax.dot_general(left, right, (((0,), (0,)), ((), ())),
                               preferred_element_type=jnp.float32)
        part = part.reshape(NT, NX, NC, 16, 512)

        @pl.when(i == 0)
        def _():
            acc[...] = part

        @pl.when(i > 0)
        def _():
            acc[...] += part

        return 0

    lax.fori_loop(0, NX, one, 0)
    swap = remote(acc.at[:, :, 1 - c], cr, cs_s.at[0], cs_r.at[0], dev(dc=1))
    swap.start()
    swap.wait_recv()
    for i in range(NX):
        obuf[i] = ((acc[:, i, c] + cr[:, i]) * scale).astype(jnp.bfloat16).reshape(64, 512)
    own_cols = pl.ds(pl.multiple_of(x * 512, 512), 512)
    for i in (2, 1, 3):
        go(remote(obuf.at[(x + i) % NX], out.at[:, own_cols], os_.at[i], or_.at[i], dev(dx=i)))
    own_o = pltpu.make_async_copy(obuf.at[x], out.at[:, own_cols], loc.at[2])
    own_o.start()
    for i in (1, 3, 2):
        from_cols = pl.ds(pl.multiple_of(((x - i) % NX) * 512, 512), 512)
        remote(obuf.at[i], out.at[:, from_cols], os_.at[i], or_.at[i], dev(dx=i)).wait_recv()
    own_o.wait()
    swap.wait_send()
    for copy in sends:
        copy.wait_send()


def of_everyone(shard, axis):
    length = lax.axis_size(axis)
    everything = lax.all_to_all(
        jnp.broadcast_to(shard[None], (length, *shard.shape)), axis, 0, 0, tiled=True
    )
    return jnp.sum(everything, axis=0)


def summed_on_arrival(shard, axis, dim):
    length = lax.axis_size(axis)
    before, after = (shard.shape[:dim], shard.shape[dim + 1 :])
    blocks = jnp.moveaxis(shard.reshape(*before, length, -1, *after), dim, 0)
    arrived = lax.all_to_all(blocks, axis, split_axis=0, concat_axis=0, tiled=True)
    return arrived.sum(axis=0)


def local(
    inputs_x,
    hidden,
    grad_up,
    grad_down,
    proj_in_up,
    proj_in_down,
    proj_out_up,
    proj_out_down,
    lengths,
    stored_grads,
):
    examples = lengths.shape[0]
    slot_count = inputs_x.shape[0] // examples
    proj_width = proj_in_up.shape[1]
    tensor_count = lax.axis_size("tensor")
    out_share = proj_width // tensor_count
    layers = 2
    terms_in = jnp.stack([matmul(inputs_x, proj_in_up), matmul(hidden, proj_in_down)])
    terms_out = jnp.stack([matmul(grad_up, proj_out_up), matmul(grad_down, proj_out_down)])
    summed_in = of_everyone(terms_in, "tensor")
    summed_out = summed_on_arrival(terms_out, "tensor", 2)
    live_mask = (jnp.arange(slot_count, dtype=jnp.int32)[None, :] < lengths[:, None]).astype(
        jnp.float32
    )
    in_proj = summed_in.reshape(layers, examples, slot_count, proj_width).transpose(1, 2, 0, 3)
    out_proj = summed_out.reshape(layers, examples, slot_count, out_share).transpose(1, 2, 0, 3)
    out_proj = out_proj * live_mask[:, :, None, None]
    current = jnp.einsum("esla,eslb->ealb", out_proj, in_proj, precision=lax.Precision.HIGHEST)
    current = (current * (1.0 / math.sqrt(slot_count))).reshape(
        examples, out_share * layers * proj_width
    )
    rows = jnp.concatenate([current.astype(jnp.bfloat16), stored_grads], axis=0)
    every_count = rows.shape[0] * lax.axis_size("dp")
    slot = 32
    rows = jnp.pad(rows, ((0, slot - rows.shape[0]), (0, 0)))
    lrow = rows.reshape(slot, NX, 512).transpose(1, 0, 2)
    rcol = rows.reshape(slot, NX, 16, 32).transpose(2, 0, 1, 3).reshape(16, slot, 128)
    vmem = pl.BlockSpec(memory_space=pltpu.VMEM)
    dma = pltpu.SemaphoreType.DMA
    owned = pl.pallas_call(
        functools.partial(exchange, 1.0 / math.sqrt(every_count)),
        out_shape=jax.ShapeDtypeStruct((64, 2048), jnp.bfloat16),
        in_specs=[vmem, vmem],
        out_specs=vmem,
        scratch_shapes=[
            pltpu.VMEM((NY, NH, NX, slot, 512), jnp.bfloat16),
            pltpu.VMEM((NX, NY * NH, slot, 512), jnp.bfloat16),
            pltpu.VMEM((NT, NX, NC, 16, 512), jnp.float32),
            pltpu.VMEM((NT, NX, 16, 512), jnp.float32),
            pltpu.VMEM((NX, 64, 512), jnp.bfloat16),
            dma((8,)), dma((8,)), dma((16,)), dma((16,)), dma((4,)), dma((4,)),
            dma((16,)), dma((16,)), dma((16,)), dma((16,)), dma((1,)), dma((1,)),
            dma((4,)), dma((4,)), dma((3,)),
        ],
        compiler_params=pltpu.CompilerParams(
            collective_id=0, has_side_effects=True, vmem_limit_bytes=40 * 1024 * 1024
        ),
        name="gram",
    )(lrow, rcol)
    return owned.T.reshape(2048, 1, 64)


def solution(mesh):
    in_specs = (
        P("dp", "tensor"),
        P("dp", "tensor"),
        P("dp", "tensor"),
        P("dp", "tensor"),
        P("tensor", None),
        P("tensor", None),
        P("tensor", None),
        P("tensor", None),
        P("dp"),
        P("dp", "tensor"),
    )
    out_specs = P("tensor", "dp", None)
    return jax.shard_map(local, mesh=mesh, in_specs=in_specs, out_specs=out_specs, check_vma=False)
```

```python
import functools
import math

import jax
import jax.numpy as jnp
from jax import lax
from jax.experimental import pallas as pl
from jax.experimental.pallas import tpu as pltpu
from jax.sharding import PartitionSpec as P

MESH = pl.DeviceIdType.MESH
NX, NY, NH, NC, NT = 4, 8, 2, 2, 4
WAVES = 2
TILE = 16


def across(left, right):
    return lax.dot_general(
        left, right, (((1,), (1,)), ((), ())), preferred_element_type=jnp.float32
    )


def exchange(scale, own, slot_scale, new_at, lengths, lst, rst, ix, hid, gu, gd, piu, pid, pou, pod,
             out, la, rb, st, lcur, rcur, acc, cr, obuf, pin, rin, pout, rout,
             vix, vhid, vgu, vgd, vpiu, vpid, vpou, vpod,
             a1s, a1r, b1s, b1r, hls, hlr, hrs, hrr, ts, tr, xs, xr, ys, yr,
             ps, pr, qs, qr, cs, cr_sem, os_, or_, loc, load):
    d = lax.axis_index("dp")
    t = lax.axis_index("tensor")
    x, y, h, c = d // 32, (d // 4) % 8, (d // 2) % 2, d % 2

    def dev(dx=0, dy=0, dh=0, dc=0, dt=0):
        xx, yy, hh, cc = (x + dx) % NX, (y + dy) % NY, (h + dh) % NH, (c + dc) % NC
        return (((xx * NY + yy) * NH + hh) * NC + cc, (t + dt) % NT)

    def remote(src, dst, ss, rs, to):
        return pltpu.make_async_remote_copy(
            src_ref=src, dst_ref=dst, send_sem=ss, recv_sem=rs, device_id=to, device_id_type=MESH
        )

    barrier = pltpu.get_barrier_semaphore()
    partners = [dev(dh=1), dev(dc=1)]
    partners += [dev(dx=i) for i in range(1, NX)] + [dev(dy=i) for i in range(1, NY)]
    partners += [dev(dt=k) for k in range(1, NT)]
    for p in partners:
        pl.semaphore_signal(barrier, inc=1, device_id=p, device_id_type=MESH)

    pairs = ((gu, vgu), (pou, vpou), (gd, vgd), (pod, vpod),
             (hid, vhid), (pid, vpid), (ix, vix), (piu, vpiu))
    loads = [pltpu.make_async_copy(a, b, load.at[i]) for i, (a, b) in enumerate(pairs)]
    for copy in loads:
        copy.start()

    sends = []

    def go(copy):
        copy.start()
        sends.append(copy)

    def lanes(k):
        return pl.ds(pl.multiple_of(((t - k) % NT) * 128, 128), 128)

    def half(j):
        return (h + j) % NH

    def l_from(w):
        return lst.at[0] if w == 0 else lcur

    def r_from(w):
        return rst.at[0] if w == 0 else rcur

    def own_copies(w):
        l, r = l_from(w), r_from(w)
        return [
            pltpu.make_async_copy(l.at[x], la.at[w, y, h, x], loc.at[w * 3]),
            pltpu.make_async_copy(
                r.at[y, h], rb.at[w, x, y, h, :, lanes(0)], loc.at[w * 3 + 1]),
            pltpu.make_async_copy(r.at[y, 1 - h], st.at[w, y], loc.at[w * 3 + 2]),
        ]

    def a1(w, i, at):
        return remote(l_from(w).at[(x + i) % NX], la.at[w, y, h, (x - at) % NX],
                      a1s.at[w * 4 + i], a1r.at[w * 4 + i], dev(dx=i))

    def b1(w, j, i, at):
        n = (w * 2 + j) * 8 + i
        yy = (y - at) % NY
        dst = st.at[w, yy] if j else rb.at[w, x, yy, h, :, lanes(0)]
        return remote(r_from(w).at[(y + i) % NY, half(j)], dst, b1s.at[n], b1r.at[n], dev(dy=i))

    def start(w):
        mine = own_copies(w)
        for copy in mine:
            copy.start()
        for i in (2, 1, 3):
            go(a1(w, i, 0))
        for j in (1, 0):
            for i in (4, 3, 5, 2, 6, 1, 7):
                go(b1(w, j, i, 0))
        return mine

    def y_copy(w, way, j, s, at):
        sign = 1 - 2 * way
        ref = la.at[w, (y - sign * at) % NY, half(j)]
        n = ((w * 2 + way) * 2 + j) * 4 + s
        return remote(ref, ref, ys.at[n], yr.at[n], dev(dy=sign))

    def y_start(w, j):
        for way in range(2):
            go(y_copy(w, way, j, 0, 0))

    def y_step(w, j, s):
        for way in range(2):
            last = 3 if way == j else 2
            if s <= last:
                y_copy(w, way, j, s, s + 1).wait_recv()
                if s + 1 <= last:
                    go(y_copy(w, way, j, s + 1, s + 1))

    def x_copy(w, way, k, j, s, at):
        sign = 1 - 2 * way
        ref = rb.at[w, (x - sign * at) % NX, :, half(j), :, lanes(k)]
        n = (((w * 2 + way) * 4 + k) * 2 + j) * 2 + s
        return remote(ref, ref, xs.at[n], xr.at[n], dev(dx=sign))

    def x_start(w, k, j):
        for way in range(2):
            go(x_copy(w, way, k, j, 0, 0))

    def x_step(w, k, j):
        for way in range(2):
            x_copy(w, way, k, j, 0, 1).wait_recv()
            if way == j:
                go(x_copy(w, way, k, j, 1, 1))

    def x_end(w, k, j):
        x_copy(w, j, k, j, 1, 2).wait_recv()

    def t_copy(w, k, j, at):
        ref = rb.at[w, x, :, half(j), :, lanes(at)]
        n = (w * 4 + k) * 2 + j
        return remote(ref, ref, ts.at[n], tr.at[n], dev(dt=k))

    def t_start(w, j):
        for k in range(1, NT):
            go(t_copy(w, k, j, 0))
        x_start(w, 0, j)

    def t_step(w, k, j):
        t_copy(w, k, j, k).wait_recv()
        x_start(w, k, j)

    def hl(w, j):
        ref = la.at[w, y, half(j)]
        return remote(ref, ref, hls.at[w], hlr.at[w], dev(dh=1))

    def hr(w, j):
        return remote(st.at[w], rb.at[w, x, :, half(j), :, lanes(0)], hrs.at[w], hrr.at[w],
                      dev(dh=1))

    def s1(w, mine):
        mine[0].wait()
        for i in range(1, NX):
            a1(w, i, i).wait_recv()
        go(hl(w, 0))
        y_start(w, 0)

    def s2(w, mine):
        mine[2].wait()
        for i in range(1, NY):
            b1(w, 1, i, i).wait_recv()
        go(hr(w, 0))
        mine[1].wait()
        for i in range(1, NY):
            b1(w, 0, i, i).wait_recv()
        t_start(w, 0)

    def s3(w):
        hl(w, 1).wait_recv()
        y_start(w, 1)

    def s4(w):
        hr(w, 1).wait_recv()
        t_start(w, 1)

    for i in range(4):
        loads[i].wait()
    for l, (g, p) in enumerate(((vgu, vpou), (vgd, vpod))):
        pout[:, l] = across(p[...], g[...]).reshape(NT, 16, 128)
    for i in range(4, 8):
        loads[i].wait()
    pin[...] = jnp.concatenate(
        [across(vix[...], vpiu[...]), across(vhid[...], vpid[...])], axis=1)

    pl.semaphore_wait(barrier, len(partners))
    for k in range(1, NT):
        go(remote(pout.at[(t + k) % NT], rout.at[k], qs.at[k], qr.at[k], dev(dt=k)))
        go(remote(pin, rin.at[k], ps.at[k], pr.at[k], dev(dt=k)))
    first = start(0)

    def current():
        for k in range(1, NT):
            remote(pout.at[k], rout.at[k], qs.at[k], qr.at[k], dev(dt=k)).wait_recv()
            remote(pin, rin.at[k], ps.at[k], pr.at[k], dev(dt=k)).wait_recv()
        summed_in = pin[...] + rin[1] + rin[2] + rin[3]
        summed_out = pout[t] + rout[1] + rout[2] + rout[3]
        token = lax.broadcasted_iota(jnp.int32, (1, 1, 128), 2)
        masked = []
        for e in range(2):
            live = (token >= e * own) & (token < e * own + lengths[e])
            masked.append(jnp.where(live, summed_out, 0.0))
        left = jnp.concatenate(masked, axis=0).reshape(64, 128)
        product = lax.dot_general(
            left, summed_in, (((1,), (0,)), ((), ())),
            precision=lax.Precision.HIGHEST, preferred_element_type=jnp.float32,
        ) * slot_scale
        product = product.reshape(2, 2, 16, 128)
        lane = lax.broadcasted_iota(jnp.int32, (16, 128), 1)
        row = lax.broadcasted_iota(jnp.int32, (16, 128), 0)
        group = lane // 32
        kept = []
        for e in range(2):
            kept.append(jnp.where(lane < 64, product[e, 0], product[e, 1]))
        for a in range(16):
            block = lst[1, a // 4, :, (a % 4) * 128:(a % 4 + 1) * 128].astype(jnp.float32)
            for e in range(2):
                block = jnp.where(row == new_at + e, kept[e][a:a + 1, :], block)
            lcur[a // 4, :, (a % 4) * 128:(a % 4 + 1) * 128] = block.astype(jnp.bfloat16)
        moved = [[kept[e] if s == 0 else pltpu.roll(kept[e], 32 * s, 1) for s in range(4)]
                 for e in range(2)]
        for g in range(16):
            u, v = g // 4, g % 4
            block = rst[1, g // 2, g % 2].astype(jnp.float32)
            for e in range(2):
                picked = moved[e][(0 - v) % 4][u:u + 1, :]
                for b in range(1, 4):
                    picked = jnp.where(group[0:1] == b,
                                       moved[e][(b - v) % 4][4 * b + u:4 * b + u + 1, :], picked)
                block = jnp.where(row == new_at + e, picked, block)
            rcur[g // 2, g % 2] = block.astype(jnp.bfloat16)

    def contract(w):
        def one(i, _):
            left = rb[w, i].reshape(16 * TILE, 512)
            right = la[w, :, :, i].reshape(16 * TILE, 512)
            part = lax.dot_general(left, right, (((0,), (0,)), ((), ())),
                                   preferred_element_type=jnp.float32)
            acc[...] += part.reshape(NT, NX, NC, 16, 512)
            return 0

        lax.fori_loop(0, NX, one, 0)

    s1(0, first)
    s2(0, first)
    y_step(0, 0, 0)
    s3(0)
    s4(0)
    current()
    second = start(1)
    acc[...] = jnp.zeros_like(acc)

    def steps(w):
        yield lambda: (x_step(w, 0, 0), t_step(w, 1, 0), t_step(w, 3, 0), t_step(w, 2, 0))
        yield lambda: (y_step(w, 0, 1), y_step(w, 1, 0))
        yield lambda: (x_step(w, 0, 1), t_step(w, 1, 1), t_step(w, 3, 1), t_step(w, 2, 1))
        yield lambda: (y_step(w, 0, 2), y_step(w, 1, 1))
        yield lambda: (x_step(w, 1, 0), x_step(w, 3, 0), x_step(w, 2, 0))
        yield lambda: (y_step(w, 0, 3), y_step(w, 1, 2))
        yield lambda: (x_step(w, 1, 1), x_step(w, 3, 1), x_step(w, 2, 1))
        yield lambda: y_step(w, 1, 3)
        yield lambda: [x_end(w, k, j) for k in (0, 1, 3, 2) for j in range(2)]

    zero, late = list(steps(0)), list(steps(1))
    zero[0]()
    zero[1]()
    s1(1, second)
    zero[2]()
    s2(1, second)
    zero[3]()
    zero[4]()
    y_step(1, 0, 0)
    s3(1)
    s4(1)
    zero[5]()
    late[0]()
    zero[6]()
    late[1]()
    zero[7]()
    late[2]()
    zero[8]()
    late[3]()
    late[4]()
    contract(0)
    for step in late[5:]:
        step()
    contract(1)

    swap = remote(acc.at[:, :, 1 - c], cr, cs.at[0], cr_sem.at[0], dev(dc=1))
    swap.start()
    swap.wait_recv()
    for i in range(NX):
        obuf[i] = ((acc[:, i, c] + cr[:, i]) * scale).astype(jnp.bfloat16).reshape(64, 512)
    own_cols = pl.ds(pl.multiple_of(x * 512, 512), 512)
    for i in (2, 1, 3):
        go(remote(obuf.at[(x + i) % NX], out.at[:, own_cols], os_.at[i], or_.at[i], dev(dx=i)))
    own_o = pltpu.make_async_copy(obuf.at[x], out.at[:, own_cols], loc.at[6])
    own_o.start()
    for i in (1, 3, 2):
        from_cols = pl.ds(pl.multiple_of(((x - i) % NX) * 512, 512), 512)
        remote(obuf.at[i], out.at[:, from_cols], os_.at[i], or_.at[i], dev(dx=i)).wait_recv()
    own_o.wait()
    swap.wait_send()
    for copy in sends:
        copy.wait_send()


def local(
    inputs_x,
    hidden,
    grad_up,
    grad_down,
    proj_in_up,
    proj_in_down,
    proj_out_up,
    proj_out_down,
    lengths,
    stored_grads,
):
    examples = lengths.shape[0]
    slot_count = inputs_x.shape[0] // examples
    stored = stored_grads.shape[0]
    every_count = (stored + examples) * lax.axis_size("dp")
    rows = jnp.pad(stored_grads, ((0, WAVES * TILE - stored), (0, 0)))
    lst = rows.reshape(WAVES, TILE, NX, 512).transpose(0, 2, 1, 3)
    rst = rows.reshape(WAVES, TILE, NX, NY, NH, 32).transpose(0, 3, 4, 1, 2, 5)
    rst = rst.reshape(WAVES, NY, NH, TILE, 128)
    vmem = pl.BlockSpec(memory_space=pltpu.VMEM)
    smem = pl.BlockSpec(memory_space=pltpu.SMEM)
    hbm = pl.BlockSpec(memory_space=pltpu.HBM)
    dma = pltpu.SemaphoreType.DMA
    bf16, f32 = jnp.bfloat16, jnp.float32
    big = [inputs_x, hidden, grad_up, grad_down,
           proj_in_up.T, proj_in_down.T, proj_out_up.T, proj_out_down.T]
    owned = pl.pallas_call(
        functools.partial(exchange, 1.0 / math.sqrt(every_count), slot_count,
                          1.0 / math.sqrt(slot_count), stored - TILE),
        out_shape=jax.ShapeDtypeStruct((64, 2048), bf16),
        in_specs=[smem, vmem, vmem] + [hbm] * 8,
        out_specs=vmem,
        scratch_shapes=[
            pltpu.VMEM((WAVES, NY, NH, NX, TILE, 512), bf16),
            pltpu.VMEM((WAVES, NX, NY, NH, TILE, 512), bf16),
            pltpu.VMEM((WAVES, NY, TILE, 128), bf16),
            pltpu.VMEM((NX, TILE, 512), bf16),
            pltpu.VMEM((NY, NH, TILE, 128), bf16),
            pltpu.VMEM((NT, NX, NC, 16, 512), f32),
            pltpu.VMEM((NT, NX, 16, 512), f32),
            pltpu.VMEM((NX, 64, 512), bf16),
            pltpu.VMEM((128, 128), f32),
            pltpu.VMEM((NT, 128, 128), f32),
            pltpu.VMEM((NT, 2, 16, 128), f32),
            pltpu.VMEM((NT, 2, 16, 128), f32),
        ]
        + [pltpu.VMEM(a.shape, bf16) for a in big]
        + [dma((n,)) for n in (8, 8, 32, 32, 2, 2, 2, 2, 16, 16, 64, 64, 32, 32,
                               4, 4, 4, 4, 1, 1, 4, 4, 7, 8)],
        compiler_params=pltpu.CompilerParams(
            collective_id=0, has_side_effects=True, vmem_limit_bytes=40 * 1024 * 1024
        ),
        name="gram",
    )(lengths, lst, rst, *big)
    return owned.T.reshape(2048, 1, 64)


def solution(mesh):
    in_specs = (
        P("dp", "tensor"),
        P("dp", "tensor"),
        P("dp", "tensor"),
        P("dp", "tensor"),
        P("tensor", None),
        P("tensor", None),
        P("tensor", None),
        P("tensor", None),
        P("dp"),
        P("dp", "tensor"),
    )
    out_specs = P("tensor", "dp", None)
    return jax.shard_map(local, mesh=mesh, in_specs=in_specs, out_specs=out_specs, check_vma=False)
```
